32 devices in a mesh: seq: 8 (over z, y), ch: 4 (over x, core).
Axes of the slice: x: 2, y: 2, z: 4, core: 2. Of those that a mesh axis runs over, the one named last changes fastest.
Arguments:
- signal: float32 [1, 65536, 1024], P(None, 'seq', 'ch'), may hold values from -6 to 6
- spectrum: float32 [2, 256, 256, 1024], P(None, 'seq', None, 'ch'), may hold values from -6 to 6
- channel_mode: int32 [1024], P('ch'), may hold values 0 or 1
- skip_gain: float32 [1024], P('ch'), may hold values from -4 to 4
- out_weight: bfloat16 [1024, 1024], P('ch'), may hold values from -0.1875 to 0.1875
Outputs:
- projected: float32 [1, 65536, 1024], P(None, 'seq', 'ch')
The draws below stay inside these ranges and needn't reach their ends.
Inputs may be any that keep to these rules, and one draw needn't show every extreme that they name: `channel_mode`: 1 marks a channel whose 65536 positions are one sequence, 0 a channel whose positions form a 256 x 256 image.
All inputs are finite; a program needn't handle non-finite values. No bound on the sum of `channel_mode` on one device may be relied on, other than what follows from the above.
Results may differ from the reference program's by a relative error of at most 0.017.
Values may be sent and summed in bfloat16 or wider, within the bound.
A program may use at most 192 MiB of HBM per device.

```python
import jax
import jax.numpy as jnp
from jax import lax

BATCH = 1
WIDTH = 1024
ROWS = 256
COLUMNS = 256
LENGTH = 65536
N_CH = 4


def place_ends(values, key, low, high):
    place = [jax.random.randint(jax.random.fold_in(key, axis), (), 0, length) for axis, length in enumerate(values.shape)]
    main_axis = values.shape.index(max(values.shape))
    neighbour = place[:main_axis] + [(place[main_axis] + 1) % values.shape[main_axis]] + place[main_axis + 1:]
    return values.at[tuple(place)].set(low).at[tuple(neighbour)].set(high)


def levels(rng, extent, shards, smallest, largest):
    def one(position, shards_of):
        steps = jax.random.uniform(jax.random.fold_in(jax.random.fold_in(rng, 6), position), (shards_of,), jnp.float32, smallest / len(shards), largest / len(shards))
        return jnp.repeat(jnp.exp(steps), extent[position] // shards_of).reshape((-1,) + (1,) * (len(extent) - position - 1))

    level = one(*shards[0])
    for cut in shards[1:]:
        level = level * one(*cut)
    return level


def centred(stream_key, dims, width, limit, cuts=(), dtype=jnp.bfloat16):
    drawn = width * jax.random.normal(stream_key, dims, jnp.float32)
    if cuts:
        drawn = drawn * levels(stream_key, dims, cuts, -0.22, 0.18)
    return jnp.clip(drawn, -limit, limit).astype(dtype)


def setup_inputs(seed: int = 0) -> dict:
    splits = jax.random.split(jax.random.key(seed), 6)
    signal = centred(splits[0], (BATCH, LENGTH, WIDTH), 1.0, 6.0, ((1, 8), (2, 4)), jnp.float32)
    spectrum = centred(splits[1], (2, ROWS, COLUMNS, WIDTH), 0.7071, 6.0, ((1, 8), (3, 4)), jnp.float32)
    channel_mode = place_ends((jax.random.randint(splits[2], (WIDTH,), 0, 2) < 1).astype(jnp.int32), jax.random.fold_in(splits[2], 1), 0, 1)
    skip_gain = centred(splits[3], (WIDTH,), 1.0, 4.0, ((0, 4),), jnp.float32)
    out_weight = centred(splits[4], (WIDTH, WIDTH), WIDTH ** -0.5, 0.1875, ((0, 4),))
    return {"signal": signal, "spectrum": spectrum, "channel_mode": channel_mode, "skip_gain": skip_gain, "out_weight": out_weight}


def convolve_block(packed):
    signal_block, spectrum_block, mode_block, gain_block = packed
    series = jnp.transpose(signal_block, (0, 2, 1))
    filters = lax.complex(spectrum_block[0], spectrum_block[1])
    filters = jnp.transpose(filters, (2, 0, 1))
    linear_filter = jnp.transpose(filters, (0, 2, 1)).reshape(filters.shape[0], LENGTH)
    linear = jnp.real(jnp.fft.ifft(jnp.fft.fft(series, axis=-1) * linear_filter[None], axis=-1))
    images = series.reshape(series.shape[0], series.shape[1], ROWS, COLUMNS)
    planar = jnp.real(jnp.fft.ifft2(jnp.fft.fft2(images, axes=(-2, -1)) * filters[None], axes=(-2, -1)))
    planar = planar.reshape(series.shape)
    convolved = jnp.where(mode_block[None, :, None] == 1, linear, planar)
    hidden = convolved + gain_block[None, :, None] * series
    return jnp.transpose(hidden, (0, 2, 1)).astype(jnp.float32)


def reference(signal, spectrum, channel_mode, skip_gain, out_weight):
    block_width = WIDTH // N_CH
    signal_parts = jnp.moveaxis(signal.reshape(BATCH, LENGTH, N_CH, block_width), 2, 0)
    spectrum_parts = jnp.moveaxis(spectrum.reshape(2, ROWS, COLUMNS, N_CH, block_width), 3, 0)
    mode_parts = channel_mode.reshape(N_CH, block_width)
    gain_parts = skip_gain.reshape(N_CH, block_width)
    hidden_parts = lax.map(convolve_block, (signal_parts, spectrum_parts, mode_parts, gain_parts))
    hidden_parts = hidden_parts.astype(jnp.bfloat16)
    weight_parts = out_weight.reshape(N_CH, block_width, WIDTH)

    def add_block(running, packed):
        features, weights = packed
        partial_value = jnp.dot(features.reshape(BATCH * LENGTH, block_width), weights, preferred_element_type=jnp.float32)
        partial_value = lax.optimization_barrier(partial_value.astype(jnp.bfloat16))
        return running + partial_value.astype(jnp.float32), jnp.zeros((), jnp.float32)

    initial = jnp.zeros((BATCH * LENGTH, WIDTH), jnp.float32)
    total, unused = lax.scan(add_block, initial, (hidden_parts, weight_parts))
    return total.reshape(BATCH, LENGTH, WIDTH)
```

```python
import math

import jax
import jax.numpy as jnp
from jax import lax
from jax.experimental import pallas as pl
from jax.experimental.pallas import tpu as pltpu
from jax.sharding import PartitionSpec as P


CHUNKS = 4


def phases(row_count, col_count, period):
    rows = jnp.arange(row_count, dtype=jnp.int32)
    cols = jnp.arange(col_count, dtype=jnp.int32)
    product = rows[:, None] * cols[None, :] % period
    angles = product.astype(jnp.float32) * (2.0 * math.pi / period)
    return jnp.cos(angles), jnp.sin(angles)


def tables(rows, columns):
    length = rows * columns
    rc, rs = phases(rows, rows, rows)
    cc, cs = phases(columns, columns, columns)
    first = jnp.concatenate([rc, -rs], 0)
    forward = jnp.concatenate(
        [jnp.concatenate([cc, -cs], 1), jnp.concatenate([cs, cc], 1)], 0
    )
    backward = jnp.concatenate(
        [jnp.concatenate([cc, cs], 1), jnp.concatenate([-cs, cc], 1)], 0
    )
    last = jnp.concatenate([rc, -rs], 1) / length
    twist_cos, twist_sin = phases(rows, columns, length)
    low = jnp.bfloat16
    return (
        first.astype(low),
        forward.astype(low),
        backward.astype(low),
        last.astype(low),
        twist_cos,
        twist_sin,
    )


def conv_kernel(
    mode_ref, x_ref, first_ref, forward_ref, backward_ref, last_ref, tc_ref, ts_ref, out_ref
):
    rows, columns = tc_ref.shape
    low = jnp.bfloat16

    def dot(a, b):
        return jnp.dot(a, b, preferred_element_type=jnp.float32)

    linear = mode_ref[pl.program_id(0)] == 1
    tc = jnp.where(linear, tc_ref[...], 1.0)
    ts = jnp.where(linear, ts_ref[...], 0.0)
    image = x_ref[:, 0, 0].reshape(rows, columns)
    y = dot(first_ref[...], image)
    yr, yi = y[:rows], y[rows:]
    y = jnp.concatenate(
        [(yr * tc + yi * ts).astype(low), (yi * tc - yr * ts).astype(low)], 1
    )
    z = dot(y, forward_ref[...])
    zr, zi = z[:, :columns], z[:, columns:]
    fr = x_ref[:, 1, 0].reshape(rows, columns).astype(jnp.float32)
    fi = x_ref[:, 2, 0].reshape(rows, columns).astype(jnp.float32)
    g = jnp.concatenate(
        [(zr * fr - zi * fi).astype(low), (zr * fi + zi * fr).astype(low)], 1
    )
    u = dot(g, backward_ref[...])
    ur, ui = u[:, :columns], u[:, columns:]
    v = jnp.concatenate(
        [(ur * tc - ui * ts).astype(low), (ur * ts + ui * tc).astype(low)], 0
    )
    out = dot(last_ref[...], v).astype(low)
    out_ref[:, 0] = out.reshape(out_ref.shape[0], out_ref.shape[2], columns)


def convolve(modes, received, consts):
    groups, planes, share, rows_local, columns = received.shape
    rows = groups * rows_local

    def whole(table):
        return pl.BlockSpec(table.shape, lambda c, m: (0,) * table.ndim)

    flops = share * 2 * 12 * rows * rows * columns
    return pl.pallas_call(
        conv_kernel,
        grid_spec=pltpu.PrefetchScalarGridSpec(
            num_scalar_prefetch=1,
            grid=(share,),
            in_specs=[
                pl.BlockSpec(
                    (groups, planes, 1, rows_local, columns), lambda c, m: (0, 0, c, 0, 0)
                )
            ]
            + [whole(t) for t in consts],
            out_specs=pl.BlockSpec(
                (groups, 1, rows_local, columns), lambda c, m: (0, c, 0, 0)
            ),
        ),
        out_shape=jax.ShapeDtypeStruct((groups, share, rows_local, columns), jnp.bfloat16),
        compiler_params=pltpu.CompilerParams(vmem_limit_bytes=24 * 1024 * 1024),
        cost_estimate=pl.CostEstimate(
            flops=flops, bytes_accessed=8 * share * rows * columns, transcendentals=0
        ),
    )(modes, received, *consts)


def per_device(signal, spectrum, channel_mode, skip_gain, out_weight):
    groups = lax.axis_size("seq")
    position = lax.axis_index("seq")
    channels_groups = lax.axis_size("ch")
    batches, local_len, owned = signal.shape
    rows_local, columns = spectrum.shape[1], spectrum.shape[2]
    rows = rows_local * groups
    chunk = owned // CHUNKS
    share = chunk // groups
    low = jnp.bfloat16
    consts = tables(rows, columns)
    weights = lax.all_to_all(out_weight, "ch", split_axis=1, concat_axis=0, tiled=True)
    out_cols = weights.shape[1]

    def pack(j, sig, spec):
        lo = j * chunk
        sig = sig[0, :, lo : lo + chunk].reshape(1, rows_local, columns, chunk)
        both = jnp.concatenate([sig.astype(low), spec[..., lo : lo + chunk].astype(low)], 0)
        both = both.reshape(3, rows_local, columns, groups, share)
        return jnp.transpose(both, (3, 0, 4, 1, 2))

    def send(j):
        return lax.all_to_all(packed[j], "seq", split_axis=0, concat_axis=0, tiled=True)

    def finish(j, back, total):
        gain = skip_gain[j * chunk : (j + 1) * chunk].reshape(groups, share, 1, 1)
        hidden = (
            back.astype(jnp.float32) + gain * packed[j][:, 0].astype(jnp.float32)
        ).astype(low)
        hidden = hidden.reshape(chunk, rows_local, columns)
        spread = lax.all_gather(hidden, "ch", axis=0, tiled=False)
        spread = spread.reshape(channels_groups * chunk, rows_local, columns)
        part = jnp.einsum(
            "cae,cj->aej",
            spread,
            weights[:, j].reshape(channels_groups * chunk, out_cols),
            preferred_element_type=jnp.float32,
        )
        return part if total is None else lax.optimization_barrier(total) + part

    packed = []
    sig, spec = signal, spectrum
    for j in range(CHUNKS):
        block = pack(j, sig, spec)
        if j == 1:
            block, weights = lax.optimization_barrier((block, weights))
        sig, spec, block = lax.optimization_barrier((sig, spec, block))
        packed.append(block)
    weights = weights.reshape(channels_groups, CHUNKS, chunk, out_cols)

    total, back = None, None
    received = send(0)
    for j in range(CHUNKS):
        modes = lax.dynamic_slice_in_dim(
            channel_mode, j * chunk + position * share, share
        )
        following = None
        if j + 1 < CHUNKS:
            if back is not None:
                packed[j + 1], back = lax.optimization_barrier((packed[j + 1], back))
            else:
                packed[j + 1], received = lax.optimization_barrier((packed[j + 1], received))
            following = send(j + 1)
        conv = convolve(modes, received, consts)
        if following is not None:
            conv, following = lax.optimization_barrier((conv, following))
        elif back is not None:
            conv, back = lax.optimization_barrier((conv, back))
        if back is not None:
            total = finish(j - 1, back, total)
        back = lax.all_to_all(conv, "seq", split_axis=0, concat_axis=0, tiled=True)
        received = following
    total = finish(CHUNKS - 1, back, total)
    return total.reshape(batches, local_len, out_cols)


def solution(mesh):
    placed = (P(None, "seq", "ch"), P(None, "seq", None, "ch"), P("ch"), P("ch"), P("ch", None))
    return jax.shard_map(
        per_device, mesh=mesh, in_specs=placed, out_specs=P(None, "seq", "ch"), check_vma=False
    )
```
